256 devices in a mesh: vox: 32 (over x, z), frm: 8 (over y, core).
Axes of the slice: x: 4, y: 4, z: 8, core: 2. Of those that a mesh axis runs over, the one named last changes fastest.
Arguments:
- casorati: float32 [256, 1048576], P('frm', 'vox'), may hold values from -6 to 6
- start_vectors: float32 [256, 64], replicated, may hold values from -6 to 6
Outputs:
- vectors: float32 [256, 64], replicated
- filtered: float32 [256, 1048576], P('frm', 'vox')
The draws below stay inside these ranges and needn't reach their ends.
All inputs are finite; a program needn't handle non-finite values.
Results may differ from the reference program's by a relative error of at most 0.0003.
Values sent between devices are 32-bit elements; how exact they have to be, the bound alone decides.
No kernel may reach another device: no remote copies, remote signals or barrier semaphores. Data moves between devices by JAX's collectives and lax.ppermute only.
A program may use at most 64 MiB of HBM per device.

```python
import jax
import jax.numpy as jnp
from jax import lax

FRAMES = 256
VECS = 64
ITERS = 3
VOXELS = 1048576


def block_levels(key, extent, cuts, low, largest):
    factor_of = 1.0
    for axis_at, blocks in cuts:
        heights = jax.random.uniform(jax.random.fold_in(jax.random.fold_in(key, 6), axis_at), (blocks,), jnp.float32, low / len(cuts), largest / len(cuts))
        factor_of = factor_of * jnp.repeat(jnp.exp(heights), extent[axis_at] // blocks).reshape((-1,) + (1,) * (len(extent) - 1 - axis_at))
    return factor_of


def bell_draw(key, extent, scale, limit, split=(), kind=jnp.bfloat16):
    array = jax.random.normal(key, extent, jnp.float32) * scale
    if len(split) > 0:
        array = block_levels(key, extent, split, -0.22, 0.18) * array
    return jnp.clip(array, min=-limit, max=limit).astype(kind)


def setup_inputs(seed: int = 0) -> dict:
    splits = jax.random.split(jax.random.key(seed), 3)
    casorati = bell_draw(splits[0], (FRAMES, VOXELS), 1.0, 6.0, ((0, 8), (1, 32)), jnp.float32)
    start_vectors = bell_draw(splits[1], (FRAMES, VECS), 1.0, 6.0, (), jnp.float32)
    return dict(casorati=casorati, start_vectors=start_vectors)


def orthonormal(projected):
    small = jnp.dot(projected.T, projected, precision=lax.Precision.HIGHEST)
    lower = jnp.linalg.cholesky(small)
    return jax.scipy.linalg.solve_triangular(lower, projected.T, lower=True).T

def reference(casorati, start_vectors):
    high = lax.Precision.HIGHEST
    vectors = start_vectors
    for step in range(ITERS):
        image = jnp.dot(vectors.T, casorati, precision=high)
        projected = jnp.dot(casorati, image.T, precision=high)
        vectors = orthonormal(projected)
    image = jnp.dot(vectors.T, casorati, precision=high)
    filtered = casorati - jnp.dot(vectors, image, precision=high)
    return (vectors, filtered)
```

```python
import functools

import jax
import jax.numpy as jnp
from jax import lax
from jax.experimental import pallas as pl
from jax.experimental.pallas import tpu as pltpu
from jax.sharding import Mesh
from jax.sharding import PartitionSpec as P

ITERS = 3
FRAMES = 256
VECS = 64
BLOCK = 64
SIZES = dict(x=4, z=8, y=4, core=2)
FRM = ("y", "core")
VOX = ("x", "z")
NT = (((1,), (1,)), ((), ()))
PAIRS = [(i, j) for i in range(FRAMES // BLOCK) for j in range(i, FRAMES // BLOCK)]


def split(value):
    high = value.astype(jnp.bfloat16)
    low = (value - high.astype(jnp.float32)).astype(jnp.bfloat16)
    return high, low


def gram_kernel(columns_ref, packed_ref, main, cross):
    chunk = 512
    main[...] = jnp.zeros_like(main)
    cross[...] = jnp.zeros_like(cross)

    @pl.loop(0, columns_ref.shape[1] // chunk)
    def _(step):
        high, low = split(columns_ref[:, pl.ds(pl.multiple_of(step * chunk, chunk), chunk)])
        main[...] += lax.dot_general(high, high, NT, preferred_element_type=jnp.float32)
        cross[...] += lax.dot_general(high, low, NT, preferred_element_type=jnp.float32)

    total = main[...] + cross[...] + cross[...].T
    packed_ref[...] = jnp.concatenate(
        [total[i * BLOCK : (i + 1) * BLOCK, j * BLOCK : (j + 1) * BLOCK] for i, j in PAIRS], axis=1
    )


def gram_packed(columns):
    return pl.pallas_call(
        gram_kernel,
        out_shape=jax.ShapeDtypeStruct((BLOCK, BLOCK * len(PAIRS)), jnp.float32),
        in_specs=[pl.BlockSpec(memory_space=pltpu.VMEM)],
        out_specs=pl.BlockSpec(memory_space=pltpu.VMEM),
        scratch_shapes=[pltpu.VMEM((FRAMES, FRAMES), jnp.float32)] * 2,
        cost_estimate=pl.CostEstimate(flops=2 * 3 * FRAMES * FRAMES * 4096, bytes_accessed=4 << 20, transcendentals=0),
        name="gram",
    )(columns)


def inverse_factor(small):
    size = small.shape[0]
    shape = (8, 2 * size)
    sublane = lax.broadcasted_iota(jnp.int32, shape, 0)
    wide = jnp.concatenate([small, jnp.eye(size, dtype=jnp.float32)], axis=1)
    rows = [wide[8 * i : 8 * i + 8, :] for i in range(size // 8)]

    def spread_row(value, row):
        return jnp.broadcast_to(value[row : row + 1, :], shape)

    scaled = []
    for block in range(size // 8):
        held = {
            i: [jnp.broadcast_to(rows[i][:, 8 * block + t : 8 * block + t + 1], shape) for t in range(8)]
            for i in range(block, size // 8)
        }
        diagonal, mine = held[block], rows[block]
        pivots = jnp.zeros(shape, jnp.float32)
        inverses, pivot_rows, heads = [], [], []
        for t in range(8):
            pivot = spread_row(diagonal[t], t)
            pivots = jnp.where(sublane == t, pivot, pivots)
            inverse = 1.0 / pivot
            factor = jnp.where(sublane > t, diagonal[t] * inverse, 0.0)
            row = spread_row(mine, t)
            mine = mine - factor * row
            head = {}
            for j in range(t + 1, 8):
                head[j] = spread_row(diagonal[j], t)
                diagonal[j] = diagonal[j] - factor * head[j]
            inverses.append(inverse)
            pivot_rows.append(row)
            heads.append(head)
        for i in range(block + 1, size // 8):
            for t in range(8):
                factor = held[i][t] * inverses[t]
                rows[i] = rows[i] - factor * pivot_rows[t]
                for j in range(t + 1, 8):
                    held[i][j] = held[i][j] - factor * heads[t][j]
        scaled.append(mine * lax.rsqrt(pivots))
    return jnp.concatenate(scaled, axis=0)[:, size:]


def iterate_kernel(packed_ref, start_ref, turned_ref, vectors_ref, gram):
    for n, (i, j) in enumerate(PAIRS):
        block = packed_ref[:, n * BLOCK : (n + 1) * BLOCK]
        gram[i * BLOCK : (i + 1) * BLOCK, j * BLOCK : (j + 1) * BLOCK] = block
        if i != j:
            gram[j * BLOCK : (j + 1) * BLOCK, i * BLOCK : (i + 1) * BLOCK] = block.T
    dot = functools.partial(
        lax.dot_general, precision=lax.Precision.HIGHEST, preferred_element_type=jnp.float32
    )
    turned_ref[...] = start_ref[...].T

    @pl.loop(0, ITERS)
    def _(step):
        projected = dot(turned_ref[...], gram[...], NT)
        small = dot(projected, projected, NT)
        turned_ref[...] = dot(inverse_factor(small), projected, (((1,), (0,)), ((), ())))

    vectors_ref[...] = turned_ref[...].T


def iterate(packed, start):
    return pl.pallas_call(
        iterate_kernel,
        out_shape=(
            jax.ShapeDtypeStruct((VECS, FRAMES), jnp.float32),
            jax.ShapeDtypeStruct((FRAMES, VECS), jnp.float32),
        ),
        in_specs=[pl.BlockSpec(memory_space=pltpu.VMEM)] * 2,
        out_specs=(pl.BlockSpec(memory_space=pltpu.VMEM),) * 2,
        scratch_shapes=[pltpu.VMEM((FRAMES, FRAMES), jnp.float32)],
        name="iterate",
    )(packed, start)


def exchange(value, axis, mask):
    pairs = [(2 * i + 1, 2 * (i ^ mask) + 1) for i in range(SIZES[axis])]
    return lax.ppermute(value, (axis, "core"), pairs)


def total_of(packed):
    y, core = lax.axis_index("y"), lax.axis_index("core")
    value = packed + lax.ppermute(packed, "core", [(0, 1)])
    stages = [(1, (y ^ (y >> 1)) & 1), (3, (y >> 1) & 1)]
    for mask, side in stages:
        half = value.shape[0] // 2
        low, high = value[:half], value[half:]
        kept, sent = jnp.where(side == 1, high, low), jnp.where(side == 1, low, high)
        value = kept + exchange(sent, "y", mask)
    for axis, mask in (("x", 1), ("x", 3), ("z", 1), ("z", 2), ("z", 6)):
        value = value + exchange(value, axis, mask)
    for mask, side in reversed(stages):
        other = exchange(value, "y", mask)
        value = jnp.where(side == 1, jnp.concatenate([other, value]), jnp.concatenate([value, other]))
    return jnp.where(core == 1, value, lax.ppermute(value, "core", [(1, 0)]))


def filter_kernel(where_ref, vectors_ref, *refs):
    casorati_ref, filtered_ref = refs[-2:]
    high, low = split(vectors_ref[...])
    left = jnp.concatenate([high, high, low], axis=1)
    for n, image_ref in enumerate(refs[:-2]):

        @pl.when(pl.program_id(0) == n)
        def _():
            top, bottom = split(image_ref[...])
            right = jnp.concatenate([top, bottom, top], axis=0)
            filtered_ref[...] = casorati_ref[...] - jnp.dot(left, right, preferred_element_type=jnp.float32)


def filtered_of(casorati, mine, pieces):
    rows = casorati.shape[0]
    width = pieces[0][1].shape[1]
    where = jnp.stack([w for w, _ in pieces]).astype(jnp.int32)
    block = pl.BlockSpec((rows, width), lambda n, where: (0, where[n]))
    return pl.pallas_call(
        filter_kernel,
        out_shape=jax.ShapeDtypeStruct(casorati.shape, jnp.float32),
        grid_spec=pltpu.PrefetchScalarGridSpec(
            num_scalar_prefetch=1,
            grid=(len(pieces),),
            in_specs=[pl.BlockSpec((rows, VECS), lambda n, where: (0, 0))]
            + [pl.BlockSpec((VECS, width), lambda n, where: (0, 0))] * len(pieces)
            + [block],
            out_specs=block,
        ),
        cost_estimate=pl.CostEstimate(flops=2 * 3 * VECS * rows * width * len(pieces), bytes_accessed=16 << 20, transcendentals=0),
        name="subtract",
    )(where, mine, *[image for _, image in pieces], casorati)


def shift(value, step):
    return lax.ppermute(value, "y", [(i, (i + step) % SIZES["y"]) for i in range(SIZES["y"])])


def swap(value):
    return lax.ppermute(value, "core", [(0, 1), (1, 0)])


def body(casorati, start):
    y, core = lax.axis_index("y"), lax.axis_index("core")
    columns = lax.all_to_all(casorati, FRM, split_axis=1, concat_axis=0, tiled=True)
    turned, vectors = iterate(total_of(gram_packed(columns)), start)
    image = lax.dot_general(
        turned, columns, (((1,), (0,)), ((), ())), precision=lax.Precision.HIGH, preferred_element_type=jnp.float32
    )
    half = image.shape[1] // 2
    left, right = image[:, :half], image[:, half:]
    up_left, down_right = shift(left, 1), shift(right, -1)
    up_right, down_left = shift(right, 1), shift(left, -1)
    far_left, far_right = shift(up_left, 1), shift(down_right, -1)
    parts = [(0, 0, left), (0, 1, right), (-1, 0, up_left), (1, 1, down_right)]
    parts += [(-1, 1, up_right), (1, 0, down_left), (2, 0, far_left), (2, 1, far_right)]
    pieces = []
    for step, side, value in parts:
        chip = (y + step) % SIZES["y"]
        pieces.append(((chip * 2 + core) * 2 + side, value))
        pieces.append(((chip * 2 + 1 - core) * 2 + side, swap(value)))
    mine = lax.dynamic_slice_in_dim(vectors, (y * 2 + core) * casorati.shape[0], casorati.shape[0], axis=0)
    return vectors, filtered_of(casorati, mine, pieces)


def solution(mesh):
    inner = Mesh(mesh.devices.reshape(4, 8, 4, 2), ("x", "z", "y", "core"))
    return jax.shard_map(
        body,
        mesh=inner,
        in_specs=(P(FRM, VOX), P()),
        out_specs=(P(), P(FRM, VOX)),
        check_vma=False,
    )
```

```python
import functools

import jax
import jax.numpy as jnp
from jax import lax
from jax.experimental import pallas as pl
from jax.experimental.pallas import tpu as pltpu
from jax.sharding import Mesh
from jax.sharding import PartitionSpec as P


ITERS = 3
FRAMES = 256
VECS = 64
BLOCK = 64
SIZES = dict(x=4, z=8, y=4, core=2)
FRM = ("y", "core")
VOX = ("x", "z")
MEMBERS = SIZES["y"] * SIZES["core"]
NT = (((1,), (1,)), ((), ()))
PAIRS = [(i, j) for i in range(FRAMES // BLOCK) for j in range(i, FRAMES // BLOCK)]


def split(value):
    high = value.astype(jnp.bfloat16)
    low = (value - high.astype(jnp.float32)).astype(jnp.bfloat16)
    return high, low


def gram_kernel(place_ref, *refs):
    pieces, before_ref = refs[:MEMBERS], refs[MEMBERS]
    packed_ref, high_ref, low_ref, main, cross = refs[MEMBERS + 1 :]
    step, rows = pl.program_id(0), pieces[0].shape[0]

    @pl.when(step == 0)
    def _():
        main[...] = jnp.zeros_like(main)
        cross[...] = jnp.zeros_like(cross)

    for mask, piece_ref in enumerate(pieces):
        mine = pl.ds(pl.multiple_of((place_ref[0] ^ mask) * rows, rows), rows)
        high_ref[mine, :], low_ref[mine, :] = split(piece_ref[...])
    high, low = high_ref[...], low_ref[...]
    main[...] += lax.dot_general(high, high, NT, preferred_element_type=jnp.float32)
    cross[...] += lax.dot_general(high, low, NT, preferred_element_type=jnp.float32)

    @pl.when(step == pl.num_programs(0) - 1)
    def _():
        total = main[...] + cross[...] + cross[...].T
        packed_ref[...] = before_ref[...] + jnp.concatenate(
            [total[i * BLOCK : (i + 1) * BLOCK, j * BLOCK : (j + 1) * BLOCK] for i, j in PAIRS], axis=1
        )


def gram_packed(place, pieces, before):
    chunk = 512
    rows, width = pieces[0].shape
    packed = pl.BlockSpec((BLOCK, BLOCK * len(PAIRS)), lambda n, place: (0, 0))
    parts = pl.BlockSpec((FRAMES, chunk), lambda n, place: (0, n))
    return pl.pallas_call(
        gram_kernel,
        out_shape=(
            jax.ShapeDtypeStruct(before.shape, jnp.float32),
            jax.ShapeDtypeStruct((FRAMES, width), jnp.bfloat16),
            jax.ShapeDtypeStruct((FRAMES, width), jnp.bfloat16),
        ),
        grid_spec=pltpu.PrefetchScalarGridSpec(
            num_scalar_prefetch=1,
            grid=(width // chunk,),
            in_specs=[pl.BlockSpec((rows, chunk), lambda n, place: (0, n))] * MEMBERS + [packed],
            out_specs=(packed, parts, parts),
            scratch_shapes=[pltpu.VMEM((FRAMES, FRAMES), jnp.float32)] * 2,
        ),
        compiler_params=pltpu.CompilerParams(vmem_limit_bytes=60 << 20),
        cost_estimate=pl.CostEstimate(
            flops=2 * 3 * FRAMES * FRAMES * width, bytes_accessed=4 << 20, transcendentals=0
        ),
        name="gram",
    )(place, *pieces, before)


def image_kernel(turned_ref, high_ref, low_ref, image_ref):
    high, low = split(turned_ref[...])
    dot = functools.partial(jnp.dot, preferred_element_type=jnp.float32)
    image_ref[...] = dot(high, high_ref[...]) + (dot(high, low_ref[...]) + dot(low, high_ref[...]))


def image_of(turned, high, low):
    chunk = 512
    width = high.shape[1]
    parts = pl.BlockSpec((FRAMES, chunk), lambda n: (0, n))
    return pl.pallas_call(
        image_kernel,
        out_shape=jax.ShapeDtypeStruct((VECS, width), jnp.float32),
        grid=(width // chunk,),
        in_specs=[pl.BlockSpec((VECS, FRAMES), lambda n: (0, 0)), parts, parts],
        out_specs=pl.BlockSpec((VECS, chunk), lambda n: (0, n)),
        compiler_params=pltpu.CompilerParams(vmem_limit_bytes=8 << 20),
        cost_estimate=pl.CostEstimate(flops=2 * 3 * VECS * FRAMES * width, bytes_accessed=4 << 20, transcendentals=0),
        name="image",
    )(turned, high, low)


def inverse_factor(small):
    size = small.shape[0]
    shape = (8, 2 * size)
    sublane = lax.broadcasted_iota(jnp.int32, shape, 0)
    wide = jnp.concatenate([small, jnp.eye(size, dtype=jnp.float32)], axis=1)
    rows = [wide[8 * i : 8 * i + 8, :] for i in range(size // 8)]

    def spread_row(value, row):
        return jnp.broadcast_to(value[row : row + 1, :], shape)

    scaled = []
    for block in range(size // 8):
        held = {
            i: [jnp.broadcast_to(rows[i][:, 8 * block + t : 8 * block + t + 1], shape) for t in range(8)]
            for i in range(block, size // 8)
        }
        diagonal, mine = held[block], rows[block]
        pivots = jnp.zeros(shape, jnp.float32)
        inverses, pivot_rows, heads = [], [], []
        for t in range(8):
            pivot = spread_row(diagonal[t], t)
            pivots = jnp.where(sublane == t, pivot, pivots)
            inverse = 1.0 / pivot
            factor = jnp.where(sublane > t, diagonal[t] * inverse, 0.0)
            row = spread_row(mine, t)
            mine = mine - factor * row
            head = {}
            for j in range(t + 1, 8):
                head[j] = spread_row(diagonal[j], t)
                diagonal[j] = diagonal[j] - factor * head[j]
            inverses.append(inverse)
            pivot_rows.append(row)
            heads.append(head)
        for i in range(block + 1, size // 8):
            for t in range(8):
                factor = held[i][t] * inverses[t]
                rows[i] = rows[i] - factor * pivot_rows[t]
                for j in range(t + 1, 8):
                    held[i][j] = held[i][j] - factor * heads[t][j]
        scaled.append(mine * lax.rsqrt(pivots))
    return jnp.concatenate(scaled, axis=0)[:, size:]


def iterate_kernel(place_ref, packed_ref, start_ref, turned_ref, mine_ref, gram, vectors):
    for n, (i, j) in enumerate(PAIRS):
        block = packed_ref[:, n * BLOCK : (n + 1) * BLOCK]
        gram[i * BLOCK : (i + 1) * BLOCK, j * BLOCK : (j + 1) * BLOCK] = block
        if i != j:
            gram[j * BLOCK : (j + 1) * BLOCK, i * BLOCK : (i + 1) * BLOCK] = block.T
    dot = functools.partial(
        lax.dot_general, precision=lax.Precision.HIGHEST, preferred_element_type=jnp.float32
    )
    turned_ref[...] = start_ref[...]

    @pl.loop(0, ITERS)
    def _(step):
        projected = dot(turned_ref[...], gram[...], NT)
        small = dot(projected, projected, NT)
        turned_ref[...] = dot(inverse_factor(small), projected, (((1,), (0,)), ((), ())))

    vectors[...] = turned_ref[...].T
    rows = mine_ref.shape[0]
    mine_ref[...] = vectors[pl.ds(pl.multiple_of(place_ref[0] * rows, rows), rows), :]


def iterate(place, packed, turned, rows):
    vmem = pl.BlockSpec(memory_space=pltpu.VMEM)
    return pl.pallas_call(
        iterate_kernel,
        out_shape=(
            jax.ShapeDtypeStruct((VECS, FRAMES), jnp.float32),
            jax.ShapeDtypeStruct((rows, VECS), jnp.float32),
        ),
        in_specs=[pl.BlockSpec(memory_space=pltpu.SMEM), vmem, vmem],
        out_specs=(vmem, vmem),
        scratch_shapes=[pltpu.VMEM((FRAMES, FRAMES), jnp.float32), pltpu.VMEM((FRAMES, VECS), jnp.float32)],
        compiler_params=pltpu.CompilerParams(vmem_limit_bytes=8 << 20),
        cost_estimate=pl.CostEstimate(flops=1 << 30, bytes_accessed=1 << 20, transcendentals=0),
        name="iterate",
    )(place, packed, turned)


def exchange(value, axis, mask):
    pairs = [(2 * i + core, 2 * (i ^ mask) + 1 - core) for i in range(SIZES[axis]) for core in (0, 1)]
    return lax.ppermute(value, (axis, "core"), pairs)


def halves(value, side):
    half = value.shape[0] // 2
    low, high = value[:half], value[half:]
    return jnp.where(side == 1, high, low), jnp.where(side == 1, low, high)


def joined(value, other, side):
    return jnp.where(side == 1, jnp.concatenate([other, value]), jnp.concatenate([value, other]))


def exchanges(values, axis):
    found = [values[0]]
    for mask in (1, 2, 3):
        flip = 1 if mask != 3 else 0
        pairs = [(2 * i + core, 2 * (i ^ mask) + (core ^ flip)) for i in range(4) for core in (0, 1)]
        found.append(lax.ppermute(values[mask], (axis, "core"), pairs))
    return found


def total_of(packed):
    x, z, y, core = (lax.axis_index(axis) for axis in SIZES)
    lane = (core ^ x ^ (x >> 1) ^ z ^ (z >> 1) ^ y ^ (y >> 1)) & 1
    kept, sent = halves(packed, lane)
    value = kept + swap(sent)
    rows = value.shape[0] // 4
    parts = [lax.dynamic_slice_in_dim(value, (y ^ mask) * rows, rows, axis=0) for mask in range(4)]
    for axis, values in (("y", parts), ("x", None)):
        a, b, c, d = exchanges(values or [value] * 4, axis)
        value = (a + b) + (c + d)
    for mask in (1, 2, 6):
        value = value + exchange(value, "z", mask)
    a, b, c, d = exchanges([value] * 4, "y")
    odd, high = (y & 1) == 1, (y >> 1) == 1
    a, b, c, d = jnp.where(odd, b, a), jnp.where(odd, a, b), jnp.where(odd, d, c), jnp.where(odd, c, d)
    low, up = jnp.concatenate([a, b]), jnp.concatenate([c, d])
    value = jnp.where(high, jnp.concatenate([up, low]), jnp.concatenate([low, up]))
    return joined(value, swap(value), lane)


def subtract_kernel(offsets, place_ref, *refs):
    vectors_ref, images, casorati_ref, filtered_ref = refs[0], refs[1 : 1 + len(offsets)], refs[-2], refs[-1]
    high, low = split(vectors_ref[...])
    left = jnp.concatenate([high, high, low], axis=1)
    for n, image_ref in enumerate(images):

        @pl.when(pl.program_id(0) == n)
        def _():
            top, bottom = split(image_ref[...])
            right = jnp.concatenate([top, bottom, top], axis=0)
            filtered_ref[...] = casorati_ref[...] - jnp.dot(left, right, preferred_element_type=jnp.float32)


def subtract(place, mine, pieces, casorati, filtered):
    rows, width = casorati.shape[0], pieces[0][3].shape[1]
    halves = casorati.shape[1] // width // (SIZES["y"] * SIZES["core"])

    def column(n, place):
        found = 0
        for index, (up, other, half, _) in enumerate(pieces):
            chip = (place[0] // 2 + up) % SIZES["y"]
            core = place[0] % 2 if other == 0 else 1 - place[0] % 2
            found = jnp.where(n == index, (chip * 2 + core) * halves + half, found)
        return (0, found)

    block = pl.BlockSpec((rows, width), column)
    specs = [pl.BlockSpec((rows, VECS), lambda n, place: (0, 0))]
    specs += [pl.BlockSpec((VECS, width), lambda n, place: (0, 0))] * len(pieces)
    operands = [mine, *[piece[3] for piece in pieces]]
    aliases = {}
    if filtered is not None:
        aliases = {1 + len(operands): 0}
        specs.append(pl.BlockSpec(memory_space=pl.ANY))
        operands.append(filtered)
    specs.append(block)
    operands.append(casorati)
    return pl.pallas_call(
        functools.partial(subtract_kernel, pieces),
        out_shape=jax.ShapeDtypeStruct(casorati.shape, jnp.float32),
        grid_spec=pltpu.PrefetchScalarGridSpec(
            num_scalar_prefetch=1, grid=(len(pieces),), in_specs=specs, out_specs=block
        ),
        input_output_aliases=aliases,
        compiler_params=pltpu.CompilerParams(vmem_limit_bytes=12 << 20),
        cost_estimate=pl.CostEstimate(
            flops=2 * 6 * VECS * rows * width * len(pieces), bytes_accessed=len(pieces) << 20, transcendentals=0
        ),
        name="subtract",
    )(place, *operands)


def shift(value, step):
    return lax.ppermute(value, "y", [(i, (i + step) % SIZES["y"]) for i in range(SIZES["y"])])


def swap(value):
    return lax.ppermute(value, "core", [(0, 1), (1, 0)])


def body(casorati, start):
    index = lax.axis_index(FRM)
    place = index.reshape(1)
    rows, width = casorati.shape[0], casorati.shape[1] // MEMBERS // 2
    packed = jnp.zeros((BLOCK, BLOCK * len(PAIRS)), jnp.float32)
    halved = []
    gathered = []
    for half in range(2):
        pieces = []
        for mask in range(MEMBERS):
            piece = lax.dynamic_slice(casorati, (0, ((index ^ mask) * 2 + half) * width), (rows, width))
            if mask:
                piece = lax.ppermute(piece, FRM, [(i, i ^ mask) for i in range(MEMBERS)])
            pieces.append(piece)
        gathered.append(pieces)
    for pieces in gathered:
        packed, *parts = gram_packed(place, pieces, packed)
        halved.append(parts)
    turned, mine = iterate(place, total_of(packed), start.T, rows)
    left, right = (image_of(turned, *parts) for parts in halved)

    up_left, down_right = shift(left, 1), shift(right, -1)
    up_right, down_left = shift(right, 1), shift(left, -1)
    far_left, far_right = shift(up_left, 1), shift(down_right, -1)
    groups = {
        "near": [(0, 0, left), (0, 1, right)],
        "first": [(-1, 0, up_left), (1, 1, down_right)],
        "second": [(-1, 1, up_right), (1, 0, down_left)],
        "far": [(2, 0, far_left), (2, 1, far_right)],
    }
    filtered = None
    for parts in groups.values():
        pieces = [(up, 0, side, value) for up, side, value in parts]
        pieces += [(up, 1, side, swap(value)) for up, side, value in parts]
        filtered = subtract(place, mine, pieces, casorati, filtered)
    return turned.T, filtered


def solution(mesh):
    inner = Mesh(mesh.devices.reshape(4, 8, 4, 2), tuple(SIZES))
    return jax.shard_map(
        body,
        mesh=inner,
        in_specs=(P(FRM, VOX), P()),
        out_specs=(P(), P(FRM, VOX)),
        check_vma=False,
    )
```

```python
import functools

import jax
import jax.numpy as jnp
from jax import lax
from jax.experimental import pallas as pl
from jax.experimental.pallas import tpu as pltpu
from jax.sharding import Mesh
from jax.sharding import PartitionSpec as P


ITERS = 3
FRAMES = 256
VECS = 64
BLOCK = 64
SIZES = dict(x=4, z=8, y=4, core=2)
FRM = ("y", "core")
VOX = ("x", "z")
MEMBERS = SIZES["y"] * SIZES["core"]
CHUNK = 512
PARTS = (3072, 1024)
NT = (((1,), (1,)), ((), ()))
PAIRS = [(i, j) for i in range(FRAMES // BLOCK) for j in range(i, FRAMES // BLOCK)]


def split(value):
    high = value.astype(jnp.bfloat16)
    low = (value - high.astype(jnp.float32)).astype(jnp.bfloat16)
    return high, low


def gram_kernel(place_ref, *refs):
    pieces, before_ref = refs[:MEMBERS], refs[MEMBERS]
    packed_ref, high_out, low_out, columns, high, low, main, cross, in_sems, out_sems = refs[MEMBERS + 1 :]
    rows, width = pieces[0].shape
    count = width // CHUNK

    def part(n):
        return pl.ds(pl.multiple_of(n * CHUNK, CHUNK), CHUNK)

    def arrivals(n):
        return [
            pltpu.make_async_copy(
                piece_ref.at[:, part(n)],
                columns.at[pl.ds(pl.multiple_of((place_ref[0] ^ mask) * rows, rows), rows), part(n)],
                in_sems.at[n, mask],
            )
            for mask, piece_ref in enumerate(pieces)
        ]

    def departures(n):
        return [
            pltpu.make_async_copy(source.at[:, part(n)], target.at[:, part(n)], out_sems.at[n, at])
            for at, (source, target) in enumerate(((high, high_out), (low, low_out)))
        ]

    for n in range(count):
        for copy in arrivals(n):
            copy.start()
    for n in range(count):
        for copy in arrivals(n):
            copy.wait()
        first, second = split(columns[:, part(n)])
        high[:, part(n)], low[:, part(n)] = first, second
        product = lax.dot_general(first, first, NT, preferred_element_type=jnp.float32)
        mixed = lax.dot_general(first, second, NT, preferred_element_type=jnp.float32)
        main[...] = product if n == 0 else main[...] + product
        cross[...] = mixed if n == 0 else cross[...] + mixed
        for copy in departures(n):
            copy.start()
    total = main[...] + cross[...] + cross[...].T
    packed_ref[...] = before_ref[...] + jnp.concatenate(
        [total[i * BLOCK : (i + 1) * BLOCK, j * BLOCK : (j + 1) * BLOCK] for i, j in PAIRS], axis=1
    )
    for n in range(count):
        for copy in departures(n):
            copy.wait()


def in_hbm(value):
    return pltpu.with_memory_space_constraint(value, pltpu.HBM)


def gram_packed(place, pieces, before):
    _, width = pieces[0].shape
    vmem, hbm = pl.BlockSpec(memory_space=pltpu.VMEM), pl.BlockSpec(memory_space=pltpu.HBM)
    return pl.pallas_call(
        gram_kernel,
        out_shape=(
            jax.ShapeDtypeStruct(before.shape, jnp.float32),
            pltpu.HBM((FRAMES, width), jnp.bfloat16),
            pltpu.HBM((FRAMES, width), jnp.bfloat16),
        ),
        in_specs=[pl.BlockSpec(memory_space=pltpu.SMEM)] + [hbm] * MEMBERS + [vmem],
        out_specs=(vmem, hbm, hbm),
        scratch_shapes=[
            pltpu.VMEM((FRAMES, width), jnp.float32),
            pltpu.VMEM((FRAMES, width), jnp.bfloat16),
            pltpu.VMEM((FRAMES, width), jnp.bfloat16),
            pltpu.VMEM((FRAMES, FRAMES), jnp.float32),
            pltpu.VMEM((FRAMES, FRAMES), jnp.float32),
            pltpu.SemaphoreType.DMA((width // CHUNK, MEMBERS)),
            pltpu.SemaphoreType.DMA((width // CHUNK, 2)),
        ],
        compiler_params=pltpu.CompilerParams(vmem_limit_bytes=16 << 20),
        cost_estimate=pl.CostEstimate(
            flops=2 * 3 * FRAMES * FRAMES * width, bytes_accessed=4 << 20, transcendentals=0
        ),
        name="gram",
    )(place, *pieces, before)


def inverse_factor(small):
    size = small.shape[0]
    shape = (8, 2 * size)
    sublane = lax.broadcasted_iota(jnp.int32, shape, 0)
    wide = jnp.concatenate([small, jnp.eye(size, dtype=jnp.float32)], axis=1)
    rows = [wide[8 * i : 8 * i + 8, :] for i in range(size // 8)]

    def spread_row(value, row):
        return jnp.broadcast_to(value[row : row + 1, :], shape)

    scaled = []
    for block in range(size // 8):
        held = {
            i: [jnp.broadcast_to(rows[i][:, 8 * block + t : 8 * block + t + 1], shape) for t in range(8)]
            for i in range(block, size // 8)
        }
        diagonal, mine = held[block], rows[block]
        pivots = jnp.zeros(shape, jnp.float32)
        inverses, pivot_rows, heads = [], [], []
        for t in range(8):
            pivot = spread_row(diagonal[t], t)
            pivots = jnp.where(sublane == t, pivot, pivots)
            inverse = 1.0 / pivot
            factor = jnp.where(sublane > t, diagonal[t] * inverse, 0.0)
            row = spread_row(mine, t)
            mine = mine - factor * row
            head = {}
            for j in range(t + 1, 8):
                head[j] = spread_row(diagonal[j], t)
                diagonal[j] = diagonal[j] - factor * head[j]
            inverses.append(inverse)
            pivot_rows.append(row)
            heads.append(head)
        for i in range(block + 1, size // 8):
            for t in range(8):
                factor = held[i][t] * inverses[t]
                rows[i] = rows[i] - factor * pivot_rows[t]
                for j in range(t + 1, 8):
                    held[i][j] = held[i][j] - factor * heads[t][j]
        scaled.append(mine * lax.rsqrt(pivots))
    return jnp.concatenate(scaled, axis=0)[:, size:]


def iterate_kernel(place_ref, packed_ref, start_ref, *refs):
    parts = (len(refs) - 9) // 2
    sources, refs = refs[: 2 * parts], refs[2 * parts :]
    turned_ref, mine_ref, left_ref, right_ref, gram, vectors, high, low, sems = refs
    copies, offset = [], 0
    for n in range(parts):
        width = sources[2 * n].shape[1]
        for at, target in enumerate((high, low)):
            copies.append(
                pltpu.make_async_copy(
                    sources[2 * n + at], target.at[:, offset : offset + width], sems.at[n, at]
                )
            )
        offset += width
    for copy in copies:
        copy.start()
    for n, (i, j) in enumerate(PAIRS):
        block = packed_ref[:, n * BLOCK : (n + 1) * BLOCK]
        gram[i * BLOCK : (i + 1) * BLOCK, j * BLOCK : (j + 1) * BLOCK] = block
        if i != j:
            gram[j * BLOCK : (j + 1) * BLOCK, i * BLOCK : (i + 1) * BLOCK] = block.T
    dot = functools.partial(
        lax.dot_general, precision=lax.Precision.HIGHEST, preferred_element_type=jnp.float32
    )
    turned_ref[...] = start_ref[...]

    @pl.loop(0, ITERS)
    def _(step):
        projected = dot(turned_ref[...], gram[...], NT)
        small = dot(projected, projected, NT)
        turned_ref[...] = dot(inverse_factor(small), projected, (((1,), (0,)), ((), ())))

    turned = turned_ref[...]
    vectors[...] = turned.T
    rows = mine_ref.shape[0]
    mine_ref[...] = vectors[pl.ds(pl.multiple_of(place_ref[0] * rows, rows), rows), :]
    for copy in copies:
        copy.wait()
    first, second = split(turned)
    for n, image_ref in enumerate((left_ref, right_ref)):
        width = image_ref.shape[1]
        some, rest = high[:, n * width : (n + 1) * width], low[:, n * width : (n + 1) * width]
        dot = functools.partial(jnp.dot, preferred_element_type=jnp.float32)
        image_ref[...] = dot(first, some) + (dot(first, rest) + dot(second, some))


def iterate(place, packed, turned, columns, rows):
    vmem, hbm = pl.BlockSpec(memory_space=pltpu.VMEM), pl.BlockSpec(memory_space=pltpu.HBM)
    width = sum(high.shape[1] for high, _ in columns)
    image = jax.ShapeDtypeStruct((VECS, width // 2), jnp.float32)
    return pl.pallas_call(
        iterate_kernel,
        out_shape=(
            jax.ShapeDtypeStruct((VECS, FRAMES), jnp.float32),
            jax.ShapeDtypeStruct((rows, VECS), jnp.float32),
            image,
            image,
        ),
        in_specs=[pl.BlockSpec(memory_space=pltpu.SMEM), vmem, vmem] + [hbm] * 2 * len(columns),
        out_specs=(vmem,) * 4,
        scratch_shapes=[
            pltpu.VMEM((FRAMES, FRAMES), jnp.float32),
            pltpu.VMEM((FRAMES, VECS), jnp.float32),
            pltpu.VMEM((FRAMES, width), jnp.bfloat16),
            pltpu.VMEM((FRAMES, width), jnp.bfloat16),
            pltpu.SemaphoreType.DMA((len(columns), 2)),
        ],
        compiler_params=pltpu.CompilerParams(vmem_limit_bytes=16 << 20),
        cost_estimate=pl.CostEstimate(flops=1 << 30, bytes_accessed=1 << 20, transcendentals=0),
        name="iterate",
    )(place, packed, turned, *[in_hbm(part) for pair in columns for part in pair])


def exchange(value, axis, mask):
    pairs = [(2 * i + core, 2 * (i ^ mask) + 1 - core) for i in range(SIZES[axis]) for core in (0, 1)]
    return lax.ppermute(value, (axis, "core"), pairs)


def halves(value, side):
    half = value.shape[0] // 2
    low, high = value[:half], value[half:]
    return jnp.where(side == 1, high, low), jnp.where(side == 1, low, high)


def joined(value, other, side):
    return jnp.where(side == 1, jnp.concatenate([other, value]), jnp.concatenate([value, other]))


def exchanges(values, axis):
    found = [values[0]]
    for mask in (1, 2, 3):
        flip = 1 if mask != 3 else 0
        pairs = [(2 * i + core, 2 * (i ^ mask) + (core ^ flip)) for i in range(4) for core in (0, 1)]
        found.append(lax.ppermute(values[mask], (axis, "core"), pairs))
    return found


def total_of(packed):
    x, z, y, core = (lax.axis_index(axis) for axis in SIZES)
    lane = (core ^ x ^ z ^ (z >> 1) ^ y ^ (y >> 1)) & 1
    kept, sent = halves(packed, lane)
    value = kept + swap(sent)
    rows = value.shape[0] // 4
    parts = [lax.dynamic_slice_in_dim(value, (y ^ mask) * rows, rows, axis=0) for mask in range(4)]
    a, b, c, d = exchanges(parts, "y")
    value = (a + b) + (c + d)
    for axis, mask in (("x", 1), ("x", 3), ("z", 1), ("z", 2), ("z", 6)):
        value = value + exchange(value, axis, mask)
    a, b, c, d = exchanges([value] * 4, "y")
    odd, high = (y & 1) == 1, (y >> 1) == 1
    a, b, c, d = jnp.where(odd, b, a), jnp.where(odd, a, b), jnp.where(odd, d, c), jnp.where(odd, c, d)
    low, up = jnp.concatenate([a, b]), jnp.concatenate([c, d])
    value = jnp.where(high, jnp.concatenate([up, low]), jnp.concatenate([low, up]))
    return joined(value, swap(value), lane)


def subtract_kernel(offsets, place_ref, *refs):
    vectors_ref, images, casorati_ref, filtered_ref = refs[0], refs[1 : 1 + len(offsets)], refs[-2], refs[-1]
    high, low = split(vectors_ref[...])
    left = jnp.concatenate([high, high, low], axis=1)
    for n, image_ref in enumerate(images):

        @pl.when(pl.program_id(0) == n)
        def _():
            top, bottom = split(image_ref[...])
            right = jnp.concatenate([top, bottom, top], axis=0)
            filtered_ref[...] = casorati_ref[...] - jnp.dot(left, right, preferred_element_type=jnp.float32)


def subtract(place, mine, pieces, casorati, filtered):
    rows, width = casorati.shape[0], pieces[0][3].shape[1]
    halves = casorati.shape[1] // width // (SIZES["y"] * SIZES["core"])

    def column(n, place):
        found = 0
        for index, (up, other, half, _) in enumerate(pieces):
            chip = (place[0] // 2 + up) % SIZES["y"]
            core = place[0] % 2 if other == 0 else 1 - place[0] % 2
            found = jnp.where(n == index, (chip * 2 + core) * halves + half, found)
        return (0, found)

    block = pl.BlockSpec((rows, width), column)
    specs = [pl.BlockSpec((rows, VECS), lambda n, place: (0, 0))]
    specs += [pl.BlockSpec((VECS, width), lambda n, place: (0, 0))] * len(pieces)
    operands = [mine, *[piece[3] for piece in pieces]]
    aliases = {}
    if filtered is not None:
        aliases = {1 + len(operands): 0}
        specs.append(pl.BlockSpec(memory_space=pl.ANY))
        operands.append(filtered)
    specs.append(block)
    operands.append(casorati)
    return pl.pallas_call(
        functools.partial(subtract_kernel, pieces),
        out_shape=jax.ShapeDtypeStruct(casorati.shape, jnp.float32),
        grid_spec=pltpu.PrefetchScalarGridSpec(
            num_scalar_prefetch=1, grid=(len(pieces),), in_specs=specs, out_specs=block
        ),
        input_output_aliases=aliases,
        compiler_params=pltpu.CompilerParams(vmem_limit_bytes=12 << 20),
        cost_estimate=pl.CostEstimate(
            flops=2 * 6 * VECS * rows * width * len(pieces), bytes_accessed=len(pieces) << 20, transcendentals=0
        ),
        name="subtract",
    )(place, *operands)


def shift(value, step):
    return lax.ppermute(value, "y", [(i, (i + step) % SIZES["y"]) for i in range(SIZES["y"])])


def swap(value):
    return lax.ppermute(value, "core", [(0, 1), (1, 0)])


def body(casorati, start):
    index = lax.axis_index(FRM)
    place = index.reshape(1)
    rows, block = casorati.shape[0], casorati.shape[1] // MEMBERS
    packed = jnp.zeros((BLOCK, BLOCK * len(PAIRS)), jnp.float32)
    source, offset, slices, columns = casorati, 0, [], []
    for width in PARTS:
        slices.append(
            [lax.dynamic_slice(source, (0, (index ^ mask) * block + offset), (rows, width)) for mask in range(MEMBERS)]
        )
        offset += width
        source = lax.optimization_barrier((source, *slices[-1]))[0]
    for pieces in slices:
        for mask in range(1, MEMBERS):
            pieces[mask] = lax.ppermute(pieces[mask], FRM, [(i, i ^ mask) for i in range(MEMBERS)])
    for part, pieces in enumerate(slices):
        packed, *found = gram_packed(place, pieces if part else [in_hbm(piece) for piece in pieces], packed)
        columns.append(found)
    turned, mine, left, right = iterate(place, total_of(packed), start.T, columns, rows)

    up_left, down_right = shift(left, 1), shift(right, -1)
    up_right, down_left = shift(right, 1), shift(left, -1)
    groups = {
        "near": [(0, 0, left), (0, 1, right)],
        "first": [(-1, 0, up_left), (1, 1, down_right)],
        "second": [(-1, 1, up_right), (1, 0, down_left)],
    }
    for part in range(2):
        width = left.shape[1] // 2
        far = [value[:, part * width : (part + 1) * width] for value in (up_left, down_right)]
        groups[f"far{part}"] = [(2, part, shift(far[0], 1)), (2, 2 + part, shift(far[1], -1))]
    filtered = None
    for parts in groups.values():
        pieces = [(up, 0, side, value) for up, side, value in parts]
        pieces += [(up, 1, side, swap(value)) for up, side, value in parts]
        filtered = subtract(place, mine, pieces, casorati, filtered)
    return turned.T, filtered


def solution(mesh):
    inner = Mesh(mesh.devices.reshape(4, 8, 4, 2), tuple(SIZES))
    return jax.shard_map(
        body,
        mesh=inner,
        in_specs=(P(FRM, VOX), P()),
        out_specs=(P(), P(FRM, VOX)),
        check_vma=False,
    )
```
